16 devices in a mesh: dp: 2 (over z), tp: 8 (over y, x, core).
Axes of the slice: x: 2, y: 2, z: 2, core: 2. Of those that a mesh axis runs over, the one named last changes fastest.
Arguments:
- x: bfloat16 [512, 2048], P('dp'), parts along dimension 0
- ln_attn_gamma: float32 [2048], replicated
- ln_attn_beta: float32 [2048], replicated
- ln_mlp_gamma: float32 [2048], replicated
- ln_mlp_beta: float32 [2048], replicated
- w_qkv: bfloat16 [2048, 16, 3, 128], P(None, 'tp')
- w_out: bfloat16 [16, 1, 128, 2048], P('tp')
- w_up: bfloat16 [2048, 8192], P(None, 'tp')
- w_down: bfloat16 [8192, 2048], P('tp')
- k_cache: bfloat16 [512, 16, 128, 128], P('dp', 'tp'), parts along dimension 0
- v_cache: bfloat16 [512, 16, 128, 128], P('dp', 'tp'), parts along dimension 0
- positions: int32 [512], P('dp'), parts along dimension 0
Outputs:
- output 1: bfloat16 [512, 2048], P('dp'), parts along dimension 0
- output 2: bfloat16 [512, 16, 128, 128], P('dp', 'tp'), parts along dimension 0
- output 3: bfloat16 [512, 16, 128, 128], P('dp', 'tp'), parts along dimension 0
There are 2 independent parts. The reference program is written for one: setup_inputs(seed, part) draws one part's arguments, and reference() takes and returns one part's arrays. A program takes and returns all parts, laid end to end along the dimension named above; an argument that names none is the same for every part.
All inputs are finite; a program needn't handle non-finite values.
Results may differ from the reference program's by a relative error of at most 0.0110548.
Values are sent between devices in bfloat16 or wider.
A program may use at most 1 GiB of HBM per device.

```python
import math
import jax
import jax.numpy as jnp
from jax import lax

D = 2048
GROUPS = 16
QPG = 1
HEAD = 128
FF = 8192
BATCH = 256
SEQ = 128

QKV_SLOTS = QPG + 2
HALF_HEAD = HEAD // 2
SCORE_SCALE = 1.0 / math.sqrt(HEAD)
LN_EPS = 1e-5
ROPE_BASE = 10000.0
NEG_BIG = -1e30


def setup_inputs(seed: int = 0, part: int = 0) -> dict:
    shared_key, part_base = jax.random.split(jax.random.key(seed))
    shared = jax.random.split(shared_key, 8)
    local = jax.random.split(jax.random.fold_in(part_base, part), 8)
    x = jax.random.normal(local[0], (BATCH, D), jnp.float32).astype(jnp.bfloat16)
    ln_attn_gamma = 1.0 + 0.3 * jax.random.normal(shared[0], (D,), jnp.float32)
    ln_attn_beta = 0.3 * jax.random.normal(shared[1], (D,), jnp.float32)
    ln_mlp_gamma = 1.0 + 0.3 * jax.random.normal(shared[2], (D,), jnp.float32)
    ln_mlp_beta = 0.3 * jax.random.normal(shared[3], (D,), jnp.float32)
    w_qkv = (jax.random.normal(shared[4], (D, GROUPS, QKV_SLOTS, HEAD), jnp.float32) * D ** -0.5).astype(jnp.bfloat16)
    w_out = (jax.random.normal(shared[5], (GROUPS, QPG, HEAD, D), jnp.float32) * (GROUPS * QPG * HEAD) ** -0.5).astype(jnp.bfloat16)
    w_up = (jax.random.normal(shared[6], (D, FF), jnp.float32) * D ** -0.5).astype(jnp.bfloat16)
    w_down = (jax.random.normal(shared[7], (FF, D), jnp.float32) * FF ** -0.5).astype(jnp.bfloat16)
    ramp = (2.0 * jnp.arange(SEQ, dtype=jnp.float32) / SEQ - 1.0)[None, None, :, None]
    k_slope = 1.5 * jax.random.normal(local[1], (BATCH, GROUPS, 1, HEAD), jnp.float32)
    k_cache = (jax.random.normal(local[2], (BATCH, GROUPS, SEQ, HEAD), jnp.float32) + ramp * k_slope).astype(jnp.bfloat16)
    v_level = jax.random.normal(local[3], (BATCH, GROUPS, 1, HEAD), jnp.float32)
    v_slope = jax.random.normal(local[4], (BATCH, GROUPS, 1, HEAD), jnp.float32)
    v_cache = (0.5 * jax.random.normal(local[5], (BATCH, GROUPS, SEQ, HEAD), jnp.float32) + v_level + ramp * v_slope).astype(jnp.bfloat16)
    positions = jax.random.randint(local[6], (BATCH,), SEQ // 4, SEQ, dtype=jnp.int32)
    positions = positions.at[0].set(SEQ - 1).at[1].set(SEQ // 4)
    return {'x': x, 'ln_attn_gamma': ln_attn_gamma, 'ln_attn_beta': ln_attn_beta, 'ln_mlp_gamma': ln_mlp_gamma, 'ln_mlp_beta': ln_mlp_beta, 'w_qkv': w_qkv, 'w_out': w_out, 'w_up': w_up, 'w_down': w_down, 'k_cache': k_cache, 'v_cache': v_cache, 'positions': positions}


def layer_norm(act_rows, ln_gamma, ln_beta):
    rows_f32 = act_rows.astype(jnp.float32)
    row_mean = jnp.mean(rows_f32, axis=-1, keepdims=True)
    centred = rows_f32 - row_mean
    row_var = jnp.mean(centred * centred, axis=-1, keepdims=True)
    return (centred * lax.rsqrt(row_var + LN_EPS) * ln_gamma + ln_beta).astype(jnp.bfloat16)


def apply_rotary(vectors, cos_t, sin_t):
    as_f32 = vectors.astype(jnp.float32)
    lower_half = as_f32[..., :HALF_HEAD]
    upper_half = as_f32[..., HALF_HEAD:]
    return jnp.concatenate([lower_half * cos_t - upper_half * sin_t, upper_half * cos_t + lower_half * sin_t], axis=-1).astype(jnp.bfloat16)


def reference(x, ln_attn_gamma, ln_attn_beta, ln_mlp_gamma, ln_mlp_beta, w_qkv, w_out, w_up, w_down, k_cache, v_cache, positions):
    attn_in = layer_norm(x, ln_attn_gamma, ln_attn_beta)
    mlp_in = layer_norm(x, ln_mlp_gamma, ln_mlp_beta)
    qkv_rows = jnp.dot(attn_in, w_qkv.reshape(D, GROUPS * QKV_SLOTS * HEAD), preferred_element_type=jnp.float32).astype(jnp.bfloat16)
    qkv_rows = qkv_rows.reshape(BATCH, GROUPS, QKV_SLOTS, HEAD)
    inv_freq = ROPE_BASE ** (-2.0 * jnp.arange(HALF_HEAD, dtype=jnp.float32) / HEAD)
    angles = positions.astype(jnp.float32)[:, None] * inv_freq[None, :]
    cos_t = jnp.cos(angles)
    sin_t = jnp.sin(angles)
    queries = apply_rotary(qkv_rows[:, :, :QPG], cos_t[:, None, None, :], sin_t[:, None, None, :])
    new_key = apply_rotary(qkv_rows[:, :, QPG], cos_t[:, None, :], sin_t[:, None, :])
    new_value = qkv_rows[:, :, QPG + 1]
    slot_ids = jnp.arange(SEQ)
    write_mask = (slot_ids[None, :] == positions[:, None])[:, None, :, None]
    keys_all = jnp.where(write_mask, new_key[:, :, None, :], k_cache)
    values_all = jnp.where(write_mask, new_value[:, :, None, :], v_cache)
    valid_mask = slot_ids[None, :] <= positions[:, None]

    def attend_group(operands):
        q_grp, k_grp, v_grp = operands
        scores = jnp.einsum('bqh,bsh->bqs', q_grp.astype(jnp.float32), k_grp.astype(jnp.float32)) * SCORE_SCALE
        scores = jnp.where(valid_mask[:, None, :], scores, NEG_BIG)
        attn_probs = jax.nn.softmax(scores, axis=-1).astype(jnp.bfloat16)
        return jnp.einsum('bqs,bsh->bqh', attn_probs.astype(jnp.float32), v_grp.astype(jnp.float32)).astype(jnp.bfloat16)

    context = lax.map(attend_group, (jnp.moveaxis(queries, 1, 0), jnp.moveaxis(keys_all, 1, 0), jnp.moveaxis(values_all, 1, 0)))
    context = jnp.moveaxis(context, 0, 1).reshape(BATCH, GROUPS * QPG * HEAD)
    attn_out = jnp.dot(context, w_out.reshape(GROUPS * QPG * HEAD, D), preferred_element_type=jnp.float32)
    hidden = jax.nn.gelu(jnp.dot(mlp_in, w_up, preferred_element_type=jnp.float32), approximate=False).astype(jnp.bfloat16)
    mlp_out = jnp.dot(hidden, w_down, preferred_element_type=jnp.float32)
    layer_out = (x.astype(jnp.float32) + attn_out + mlp_out).astype(jnp.bfloat16)
    return (layer_out, keys_all, values_all)
```

```python
import functools
import math

import jax
import jax.numpy as jnp
import numpy as np
from jax import lax
from jax.experimental import pallas as pl
from jax.experimental.pallas import tpu as pltpu
from jax.sharding import PartitionSpec as P

LN_EPS = 1e-5
ROPE_BASE = 10000.0
NEG_BIG = -1e30
MESH = pl.DeviceIdType.MESH
F32 = jnp.float32
BF16 = jnp.bfloat16
ROWS = 16
CONTRACT_LAST = (((1,), (1,)), ((), ()))


def quad_lhs(block, tile):
    row = lax.broadcasted_iota(jnp.int32, block.shape, 0)
    zero = jnp.zeros_like(block)
    left = jnp.where((row == 4 * tile) | (row == 4 * tile + 2), block, zero)
    right = jnp.where((row == 4 * tile + 1) | (row == 4 * tile + 3), block, zero)
    return jnp.concatenate([left, right], axis=1).astype(BF16)


def pick_half(acc):
    row = lax.broadcasted_iota(jnp.int32, (acc.shape[0], 128), 0)
    return jnp.where((row & 3) < 2, acc[:, :128], acc[:, 128:])


def layer_kernel(x_hbm, g1_hbm, b1_hbm, g2_hbm, b2_hbm, freq_hbm, wqkv_hbm, wout_hbm, wup_hbm, wdown_hbm, k_hbm, v_hbm, pos_hbm,
                 part_ref, ko_hbm, vo_hbm,
                 x_ref, ln_ref, freq_ref, wraw_ref, wcat_ref, wout_ref, wup_ref, wdown_ref, kbuf, vbuf, pos_ref,
                 ain_ref, min_ref, y_ref, t_ref, q_ref, nk_ref, nv_ref, s_ref, ctx_ref, hid_ref, stage_ref,
                 sem_in, sem_w, sem_k, sem_v, sem_ko, sem_vo):
    n_rows, d_model = x_ref.shape
    n_groups = kbuf.shape[1]
    n_chunks = n_rows // ROWS
    n_wparts = 4
    wrows = wraw_ref.shape[0] // n_wparts

    def copy_small(i, src, dst):
        return pltpu.make_async_copy(src, dst, sem_in.at[i])

    smalls = [copy_small(0, pos_hbm, pos_ref), copy_small(1, x_hbm, x_ref), copy_small(2, freq_hbm, freq_ref)]
    for i, src in enumerate((g1_hbm, b1_hbm, g2_hbm, b2_hbm)):
        smalls.append(copy_small(3 + i, src, ln_ref.at[i]))
    for c in smalls:
        c.start()
    wparts = [pltpu.make_async_copy(wqkv_hbm.at[pl.ds(i * wrows, wrows)], wraw_ref.at[pl.ds(i * wrows, wrows)], sem_w.at[i])
              for i in range(n_wparts)]
    for c in wparts:
        c.start()

    def chunk_ds(i):
        return pl.ds(pl.multiple_of(i * ROWS, ROWS), ROWS)

    def k_in(i):
        return pltpu.make_async_copy(k_hbm.at[chunk_ds(i)], kbuf.at[chunk_ds(i)], sem_k.at[i])

    def v_in(i):
        return pltpu.make_async_copy(v_hbm.at[chunk_ds(i)], vbuf.at[chunk_ds(i)], sem_v.at[i])

    def k_out(i):
        return pltpu.make_async_copy(kbuf.at[chunk_ds(i)], ko_hbm.at[chunk_ds(i)], sem_ko.at[i])

    def v_out(i):
        return pltpu.make_async_copy(vbuf.at[chunk_ds(i)], vo_hbm.at[chunk_ds(i)], sem_vo.at[i])

    for i in range(n_chunks):
        k_in(i).start()
        v_in(i).start()
    wbig = [pltpu.make_async_copy(wup_hbm, wup_ref, sem_w.at[n_wparts]),
            pltpu.make_async_copy(wdown_hbm, wdown_ref, sem_w.at[n_wparts + 1]),
            pltpu.make_async_copy(wout_hbm, wout_ref, sem_w.at[n_wparts + 2])]
    for c in wbig:
        c.start()

    smalls[0].wait()
    row8 = lax.broadcasted_iota(jnp.int32, (8, 128), 0)

    @pl.loop(0, n_rows // 8)
    def _(r):
        tile = jnp.zeros((8, 128), jnp.int32)
        for j in range(8):
            tile = jnp.where(row8 == j, pos_ref[r * 8 + j], tile)
        t_ref[pl.ds(pl.multiple_of(r * 8, 8), 8), :] = tile

    for c in smalls[1:]:
        c.wait()

    gains = [ln_ref[i] for i in range(4)]

    @pl.loop(0, n_rows // 16)
    def _(r):
        rows = pl.ds(pl.multiple_of(r * 16, 16), 16)
        act = x_ref[rows, :].astype(F32)
        mean = jnp.mean(act, axis=-1, keepdims=True)
        centred = act - mean
        var = jnp.mean(centred * centred, axis=-1, keepdims=True)
        normed = centred * lax.rsqrt(var + LN_EPS)
        ain_ref[rows, :] = (normed * gains[0] + gains[1]).astype(BF16)
        min_ref[rows, :] = (normed * gains[2] + gains[3]).astype(BF16)

    depth = 64
    n_split = 3 * n_groups
    for p in range(n_wparts):
        wparts[p].wait()

        @pl.loop(0, wrows // (depth * n_split))
        def _(r):
            first = p * wrows + r * (depth * n_split)
            stage_ref[...] = wraw_ref[pl.ds(pl.multiple_of(first, depth * n_split), depth * n_split), :].astype(F32)
            feat = pl.ds(pl.multiple_of(p * (wrows // n_split) + r * depth, depth), depth)
            for slot in range(3):
                for g in range(n_groups):
                    col = (g * 3 + slot) * 128
                    wcat_ref[feat, col:col + 128] = stage_ref[pl.ds(slot * n_groups + g, depth, stride=n_split), :].astype(BF16)

    for c0 in range(0, 3 * n_groups * 128, 256):
        y_ref[:, c0:c0 + 256] = jnp.dot(ain_ref[...], wcat_ref[:, c0:c0 + 256], preferred_element_type=F32).astype(BF16).astype(F32)

    angles = t_ref[...].astype(F32) * freq_ref[...]
    cos_t = jnp.cos(angles)
    lane = lax.broadcasted_iota(jnp.int32, angles.shape, 1)
    sin_t = jnp.sin(angles)
    sin_t = jnp.where(lane < 64, -sin_t, sin_t)
    for g in range(n_groups):
        for slot, dst in ((0, q_ref), (1, nk_ref)):
            vec = y_ref[:, (g * 3 + slot) * 128:(g * 3 + slot + 1) * 128]
            turned = vec * cos_t + pltpu.roll(vec, 64, 1) * sin_t
            dst[g] = turned.astype(BF16).astype(F32)
        nv_ref[g] = y_ref[:, (g * 3 + 2) * 128:(g * 3 + 3) * 128]

    slot16 = lax.broadcasted_iota(jnp.int32, (128, 128), 0).astype(F32).astype(BF16).reshape(8, 16, 128)
    scale = 128 ** -0.5

    def put_new(buf, i, b, g, new16, pos16):
        old = buf[i * ROWS + b, g].reshape(8, 16, 128)
        new = jnp.broadcast_to(new16[b:b + 1, :], (16, 128)).astype(BF16)[None]
        at = jnp.broadcast_to(pos16[b:b + 1, :], (16, 128)).astype(BF16)[None]
        block = jnp.where(slot16 == at, new, old).reshape(128, 128)
        buf[i * ROWS + b, g] = block
        return block

    def score_chunk(i):
        k_in(i).wait()
        rows = chunk_ds(i)
        pos16 = t_ref[rows, :].astype(F32)
        for g in range(n_groups):
            new16 = nk_ref[g, rows, :]
            q16 = q_ref[g, rows, :]
            acc = None
            for tile in range(4):
                blk = [put_new(kbuf, i, 4 * tile + j, g, new16, pos16) for j in range(4)]
                rhs = jnp.concatenate([jnp.concatenate(blk[:2], axis=1), jnp.concatenate(blk[2:], axis=1)], axis=0)
                part = lax.dot_general(quad_lhs(q16, tile), rhs, CONTRACT_LAST, preferred_element_type=F32)
                acc = part if acc is None else acc + part
            s_ref[i % 2, g] = pick_half(acc) * scale
        k_out(i).start()

    def context_chunk(i):
        v_in(i).wait()
        rows = chunk_ds(i)
        pos16 = t_ref[rows, :]
        lane16 = lax.broadcasted_iota(jnp.int32, (ROWS, 128), 1)
        pos16f = pos16.astype(F32)
        for g in range(n_groups):
            sc = jnp.where(lane16 <= pos16, s_ref[i % 2, g], NEG_BIG)
            ex = jnp.exp(sc - jnp.max(sc, axis=-1, keepdims=True))
            prob = (ex / jnp.sum(ex, axis=-1, keepdims=True)).astype(BF16).astype(F32)
            new16 = nv_ref[g, rows, :]
            acc = None
            for tile in range(4):
                blk = [put_new(vbuf, i, 4 * tile + j, g, new16, pos16f) for j in range(4)]
                rhs = jnp.concatenate([jnp.concatenate(blk[0::2], axis=1), jnp.concatenate(blk[1::2], axis=1)], axis=0)
                part = jnp.dot(quad_lhs(prob, tile), rhs, preferred_element_type=F32)
                acc = part if acc is None else acc + part
            ctx_ref[rows, g * 128:(g + 1) * 128] = pick_half(acc).astype(BF16)
        v_out(i).start()

    score_chunk(0)

    @pl.loop(1, n_chunks)
    def _(i):
        score_chunk(i)
        context_chunk(i - 1)

    context_chunk(n_chunks - 1)

    wbig[0].wait()

    @pl.loop(0, wup_ref.shape[1] // 256)
    def _(c):
        cols = pl.ds(pl.multiple_of(c * 256, 256), 256)
        up = jnp.dot(min_ref[...], wup_ref[:, cols], preferred_element_type=F32)
        hid_ref[:, cols] = (0.5 * up * (1.0 + lax.erf(up * math.sqrt(0.5)))).astype(BF16)

    wbig[1].wait()
    wbig[2].wait()

    @pl.loop(0, d_model // 256)
    def _(c):
        cols = pl.ds(pl.multiple_of(c * 256, 256), 256)
        total = jnp.dot(hid_ref[...], wdown_ref[:, cols], preferred_element_type=F32)
        total = total + jnp.dot(ctx_ref[...], wout_ref[:, cols], preferred_element_type=F32)
        part_ref[:, cols] = total.astype(BF16)

    @pl.loop(0, n_chunks)
    def _(i):
        k_out(i).wait()
        v_out(i).wait()


N_COL = 4


def reduce_kernel(part_ref, x_hbm, out_ref, d_recv, a_send, a_recv, b_send, b_recv, keep, x_ref,
                  x_sem, d_ss, d_rs, a_ss, a_rs, b_ss, b_rs, gb_ss, gb_rs, ga_ss, ga_rs, gd_ss, gd_rs):
    me = lax.axis_index('tp')
    core = me & 1
    xpos = (me >> 1) & 1
    ypos = (me >> 2) & 1
    first_bit = jnp.where(core == 0, 2, 4)
    second_bit = 6 - first_bit
    first = me ^ first_bit
    second = me ^ second_bit
    partner = me ^ 1
    first_pos = jnp.where(core == 0, xpos, ypos)
    second_pos = jnp.where(core == 0, ypos, xpos)
    n_rows, d_model = part_ref.shape
    half, quarter, eighth = n_rows // 2, n_rows // 4, n_rows // 8
    width = d_model // N_COL

    def rows(start, size):
        return pl.ds(pl.multiple_of(start, eighth), size)

    def cols(j):
        return pl.ds(j * width, width)

    mine_half = core * half
    mine_quarter = mine_half + first_pos * quarter
    mine = mine_quarter + second_pos * eighth
    their_quarter = mine_half + (1 - first_pos) * quarter
    second_rows = mine_quarter + (1 - second_pos) * eighth

    def remote(src, dst, ss, rs, dev):
        return pltpu.make_async_remote_copy(src_ref=src, dst_ref=dst, send_sem=ss, recv_sem=rs, device_id={'tp': dev}, device_id_type=MESH)

    x_copy = pltpu.make_async_copy(x_hbm.at[rows(mine, eighth)], x_ref, x_sem)
    x_copy.start()
    barrier = pltpu.get_barrier_semaphore()
    for dev in (partner, first, second):
        pl.semaphore_signal(barrier, inc=1, device_id={'tp': dev}, device_id_type=MESH)
    pl.semaphore_wait(barrier, 3)

    d_copies, a_copies, b_copies = [], [], []
    for j in range(N_COL):
        c = remote(part_ref.at[rows((1 - core) * half, half), cols(j)], d_recv.at[:, cols(j)], d_ss.at[j], d_rs.at[j], partner)
        c.start()
        d_copies.append(c)
    for j in range(N_COL):
        d_copies[j].wait_recv()
        go = part_ref[rows(their_quarter, quarter), cols(j)].astype(F32) + d_recv[rows((1 - first_pos) * quarter, quarter), cols(j)].astype(F32)
        a_send[:, cols(j)] = go.astype(BF16)
        c = remote(a_send.at[:, cols(j)], a_recv.at[:, cols(j)], a_ss.at[j], a_rs.at[j], first)
        c.start()
        a_copies.append(c)
        keep[:, cols(j)] = part_ref[rows(mine_quarter, quarter), cols(j)].astype(F32) + d_recv[rows(first_pos * quarter, quarter), cols(j)].astype(F32)
    for j in range(N_COL):
        a_copies[j].wait_recv()
        away = rows((1 - second_pos) * eighth, eighth)
        b_send[:, cols(j)] = (keep[away, cols(j)] + a_recv[away, cols(j)].astype(F32)).astype(BF16)
        c = remote(b_send.at[:, cols(j)], b_recv.at[:, cols(j)], b_ss.at[j], b_rs.at[j], second)
        c.start()
        b_copies.append(c)
    x_copy.wait()
    gathers = []
    for j in range(N_COL):
        b_copies[j].wait_recv()
        home = rows(second_pos * eighth, eighth)
        total = keep[home, cols(j)] + a_recv[home, cols(j)].astype(F32) + b_recv[:, cols(j)].astype(F32) + x_ref[:, cols(j)].astype(F32)
        out_ref[rows(mine, eighth), cols(j)] = total.astype(BF16)
        block = out_ref.at[rows(mine, eighth), cols(j)]
        sends = [remote(block, block, gb_ss.at[j], gb_rs.at[j], second),
                 remote(block, block, ga_ss.at[j, 0], ga_rs.at[j, 0], first),
                 remote(block, block, gd_ss.at[j, 0], gd_rs.at[j, 0], partner)]
        for c in sends:
            c.start()
        gathers.append(sends)
    for j in range(N_COL):
        gathers[j][0].wait_recv()
        block = out_ref.at[rows(second_rows, eighth), cols(j)]
        sends = [remote(block, block, ga_ss.at[j, 1], ga_rs.at[j, 1], first),
                 remote(block, block, gd_ss.at[j, 1], gd_rs.at[j, 1], partner)]
        for c in sends:
            c.start()
        gathers[j] += sends
    for j in range(N_COL):
        gathers[j][1].wait_recv()
        gathers[j][3].wait_recv()
        block = out_ref.at[rows(their_quarter, quarter), cols(j)]
        c = remote(block, block, gd_ss.at[j, 2], gd_rs.at[j, 2], partner)
        c.start()
        gathers[j].append(c)
    for j in range(N_COL):
        gathers[j][2].wait_recv()
        gathers[j][4].wait_recv()
        gathers[j][5].wait_recv()
    for j in range(N_COL):
        d_copies[j].wait_send()
        a_copies[j].wait_send()
        b_copies[j].wait_send()
        for c in gathers[j]:
            c.wait_send()


def solution(mesh):
    row_spec = P('dp', None)
    vec_spec = P(None)
    cache_spec = P('dp', 'tp', None, None)
    hbm = pl.BlockSpec(memory_space=pl.ANY)
    vmem = pl.BlockSpec(memory_space=pltpu.VMEM)
    dma = pltpu.SemaphoreType.DMA

    def device_step(x, ln_attn_gamma, ln_attn_beta, ln_mlp_gamma, ln_mlp_beta, w_qkv, w_out, w_up, w_down, k_cache, v_cache, positions):
        n_rows, d_model = x.shape
        n_groups, seq, head = k_cache.shape[1:]
        ff = w_up.shape[1]
        n_chunks = n_rows // ROWS
        qkv_cols = n_groups * 3 * head
        freq = ROPE_BASE ** (-2.0 * np.arange(head // 2, dtype=np.float64) / head)
        freq = jnp.asarray(np.concatenate([freq, freq])[None, :], F32)
        w_rows = w_qkv.transpose(0, 2, 1, 3).reshape(d_model * n_groups * 3, head)
        lns = [v.reshape(1, d_model) for v in (ln_attn_gamma, ln_attn_beta, ln_mlp_gamma, ln_mlp_beta)]
        part, k_new, v_new = pl.pallas_call(
            layer_kernel,
            out_shape=(pltpu.VMEM((n_rows, d_model), BF16),
                       jax.ShapeDtypeStruct(k_cache.shape, k_cache.dtype),
                       jax.ShapeDtypeStruct(v_cache.shape, v_cache.dtype)),
            in_specs=[hbm] * 13,
            out_specs=(vmem, hbm, hbm),
            scratch_shapes=[
                pltpu.VMEM((n_rows, d_model), BF16),
                pltpu.VMEM((4, 1, d_model), F32),
                pltpu.VMEM((1, head), F32),
                pltpu.VMEM(w_rows.shape, BF16),
                pltpu.VMEM((d_model, qkv_cols), BF16),
                pltpu.VMEM((n_groups * head, d_model), BF16),
                pltpu.VMEM((d_model, ff), BF16),
                pltpu.VMEM((ff, d_model), BF16),
                pltpu.VMEM(k_cache.shape, BF16),
                pltpu.VMEM(v_cache.shape, BF16),
                pltpu.SMEM((n_rows,), jnp.int32),
                pltpu.VMEM((n_rows, d_model), BF16),
                pltpu.VMEM((n_rows, d_model), BF16),
                pltpu.VMEM((n_rows, qkv_cols), F32),
                pltpu.VMEM((n_rows, 128), jnp.int32),
                pltpu.VMEM((n_groups, n_rows, head), F32),
                pltpu.VMEM((n_groups, n_rows, head), F32),
                pltpu.VMEM((n_groups, n_rows, head), F32),
                pltpu.VMEM((2, n_groups, ROWS, seq), F32),
                pltpu.VMEM((n_rows, n_groups * head), BF16),
                pltpu.VMEM((n_rows, ff), BF16),
                pltpu.VMEM((64 * 3 * n_groups, head), F32),
                dma((8,)), dma((8,)), dma((n_chunks,)), dma((n_chunks,)), dma((n_chunks,)), dma((n_chunks,)),
            ],
            compiler_params=pltpu.CompilerParams(vmem_limit_bytes=60 * 1024 * 1024),
            cost_estimate=pl.CostEstimate(flops=4 * 10 ** 9, bytes_accessed=80 * 10 ** 6, transcendentals=0),
            name='layer',
        )(x, *lns, freq, w_rows, w_out.reshape(n_groups * head, d_model), w_up, w_down, k_cache, v_cache, positions)
        half, quarter, eighth = n_rows // 2, n_rows // 4, n_rows // 8
        out = pl.pallas_call(
            reduce_kernel,
            out_shape=jax.ShapeDtypeStruct((n_rows, d_model), BF16),
            in_specs=[vmem, hbm],
            out_specs=vmem,
            scratch_shapes=[
                pltpu.VMEM((half, d_model), BF16),
                pltpu.VMEM((quarter, d_model), BF16),
                pltpu.VMEM((quarter, d_model), BF16),
                pltpu.VMEM((eighth, d_model), BF16),
                pltpu.VMEM((eighth, d_model), BF16),
                pltpu.VMEM((quarter, d_model), F32),
                pltpu.VMEM((eighth, d_model), BF16),
                dma(()),
                dma((N_COL,)), dma((N_COL,)), dma((N_COL,)), dma((N_COL,)), dma((N_COL,)), dma((N_COL,)),
                dma((N_COL,)), dma((N_COL,)), dma((N_COL, 2)), dma((N_COL, 2)), dma((N_COL, 3)), dma((N_COL, 3)),
            ],
            compiler_params=pltpu.CompilerParams(collective_id=0, has_side_effects=True, vmem_limit_bytes=16 * 1024 * 1024),
            name='reduce',
        )(part, x)
        return out, k_new, v_new

    return jax.shard_map(device_step, mesh=mesh, in_specs=(row_spec, vec_spec, vec_spec, vec_spec, vec_spec, P(None, 'tp', None, None), P('tp', None, None, None), P(None, 'tp'), P('tp', None), cache_spec, cache_spec, P('dp')), out_specs=(row_spec, cache_spec, cache_spec), check_vma=False)
```

```python
import functools
import math

import jax
import jax.numpy as jnp
import numpy as np
from jax import lax
from jax.experimental import pallas as pl
from jax.experimental.pallas import tpu as pltpu
from jax.sharding import PartitionSpec as P

LN_EPS = 1e-5
ROPE_BASE = 10000.0
NEG_BIG = -1e30
MESH = pl.DeviceIdType.MESH
F32 = jnp.float32
BF16 = jnp.bfloat16
ROWS = 16
CONTRACT_LAST = (((1,), (1,)), ((), ()))


def quad_lhs(block, tile):
    row = lax.broadcasted_iota(jnp.int32, block.shape, 0)
    zero = jnp.zeros_like(block)
    left = jnp.where((row == 4 * tile) | (row == 4 * tile + 2), block, zero)
    right = jnp.where((row == 4 * tile + 1) | (row == 4 * tile + 3), block, zero)
    return jnp.concatenate([left, right], axis=1).astype(BF16)


def pick_half(acc):
    row = lax.broadcasted_iota(jnp.int32, (acc.shape[0], 128), 0)
    return jnp.where((row & 3) < 2, acc[:, :128], acc[:, 128:])


def layer_kernel(x_hbm, g1_hbm, b1_hbm, g2_hbm, b2_hbm, freq_hbm, wqkv_hbm, wout_hbm, wup_hbm, wdown_hbm, k_hbm, v_hbm, pos_hbm,
                 part_ref, ko_hbm, vo_hbm,
                 x_ref, ln_ref, freq_ref, wraw_ref, wcat_ref, wout_ref, wup_ref, wdown_ref, kbuf, vbuf, pos_ref,
                 ain_ref, min_ref, y_ref, t_ref, q_ref, nk_ref, nv_ref, s_ref, ctx_ref, hid_ref, stage_ref,
                 sem_in, sem_w, sem_k, sem_v, sem_ko, sem_vo):
    n_rows, d_model = x_ref.shape
    n_groups = kbuf.shape[1]
    n_chunks = n_rows // ROWS
    n_wparts = 4
    wrows = wraw_ref.shape[0] // n_wparts

    def copy_small(i, src, dst):
        return pltpu.make_async_copy(src, dst, sem_in.at[i])

    smalls = [copy_small(0, pos_hbm, pos_ref), copy_small(1, x_hbm, x_ref), copy_small(2, freq_hbm, freq_ref)]
    for i, src in enumerate((g1_hbm, b1_hbm, g2_hbm, b2_hbm)):
        smalls.append(copy_small(3 + i, src, ln_ref.at[i]))
    for c in smalls:
        c.start()
    wparts = [pltpu.make_async_copy(wqkv_hbm.at[pl.ds(i * wrows, wrows)], wraw_ref.at[pl.ds(i * wrows, wrows)], sem_w.at[i])
              for i in range(n_wparts)]
    for c in wparts:
        c.start()

    def chunk_ds(i):
        return pl.ds(pl.multiple_of(i * ROWS, ROWS), ROWS)

    def k_in(i):
        return pltpu.make_async_copy(k_hbm.at[chunk_ds(i)], kbuf.at[chunk_ds(i)], sem_k.at[i])

    def v_in(i):
        return pltpu.make_async_copy(v_hbm.at[chunk_ds(i)], vbuf.at[chunk_ds(i)], sem_v.at[i])

    def k_out(i):
        return pltpu.make_async_copy(kbuf.at[chunk_ds(i)], ko_hbm.at[chunk_ds(i)], sem_ko.at[i])

    def v_out(i):
        return pltpu.make_async_copy(vbuf.at[chunk_ds(i)], vo_hbm.at[chunk_ds(i)], sem_vo.at[i])

    def fetch(lo, hi):
        @pl.loop(lo, hi)
        def _(i):
            k_in(i).start()
            v_in(i).start()

    fetch(0, 2)
    wbig = [pltpu.make_async_copy(wup_hbm, wup_ref, sem_w.at[n_wparts]),
            pltpu.make_async_copy(wdown_hbm, wdown_ref, sem_w.at[n_wparts + 1]),
            pltpu.make_async_copy(wout_hbm, wout_ref, sem_w.at[n_wparts + 2])]

    smalls[0].wait()
    row8 = lax.broadcasted_iota(jnp.int32, (8, 128), 0)

    @pl.loop(0, n_rows // 8)
    def _(r):
        tile = jnp.zeros((8, 128), jnp.int32)
        for j in range(8):
            tile = jnp.where(row8 == j, pos_ref[r * 8 + j], tile)
        t_ref[pl.ds(pl.multiple_of(r * 8, 8), 8), :] = tile

    for c in smalls[1:]:
        c.wait()
    fetch(2, 5)

    gains = [ln_ref[i] for i in range(4)]

    @pl.loop(0, n_rows // 16)
    def _(r):
        rows = pl.ds(pl.multiple_of(r * 16, 16), 16)
        act = x_ref[rows, :].astype(F32)
        mean = jnp.mean(act, axis=-1, keepdims=True)
        centred = act - mean
        var = jnp.mean(centred * centred, axis=-1, keepdims=True)
        normed = centred * lax.rsqrt(var + LN_EPS)
        ain_ref[rows, :] = (normed * gains[0] + gains[1]).astype(BF16)
        min_ref[rows, :] = (normed * gains[2] + gains[3]).astype(BF16)

    fetch(5, 8)

    depth = 64
    n_split = 3 * n_groups
    for p in range(n_wparts):
        wparts[p].wait()

        @pl.loop(0, wrows // (depth * n_split))
        def _(r):
            first = p * wrows + r * (depth * n_split)
            stage_ref[...] = wraw_ref[pl.ds(pl.multiple_of(first, depth * n_split), depth * n_split), :].astype(F32)
            feat = pl.ds(pl.multiple_of(p * (wrows // n_split) + r * depth, depth), depth)
            for slot in range(3):
                for g in range(n_groups):
                    col = (g * 3 + slot) * 128
                    wcat_ref[feat, col:col + 128] = stage_ref[pl.ds(slot * n_groups + g, depth, stride=n_split), :].astype(BF16)

        fetch(8 + p, 9 + p)

    for c in wbig:
        c.start()
    fetch(12, n_chunks)

    for c0 in range(0, 3 * n_groups * 128, 256):
        y_ref[:, c0:c0 + 256] = jnp.dot(ain_ref[...], wcat_ref[:, c0:c0 + 256], preferred_element_type=F32).astype(BF16).astype(F32)

    angles = t_ref[...].astype(F32) * freq_ref[...]
    cos_t = jnp.cos(angles)
    lane = lax.broadcasted_iota(jnp.int32, angles.shape, 1)
    sin_t = jnp.sin(angles)
    sin_t = jnp.where(lane < 64, -sin_t, sin_t)
    for g in range(n_groups):
        for slot, dst in ((0, q_ref), (1, nk_ref)):
            vec = y_ref[:, (g * 3 + slot) * 128:(g * 3 + slot + 1) * 128]
            turned = vec * cos_t + pltpu.roll(vec, 64, 1) * sin_t
            dst[g] = turned.astype(BF16).astype(F32)
        nv_ref[g] = y_ref[:, (g * 3 + 2) * 128:(g * 3 + 3) * 128]

    slot16 = lax.broadcasted_iota(jnp.int32, (128, 128), 0).astype(F32).astype(BF16).reshape(8, 16, 128)
    scale = 128 ** -0.5

    def put_new(buf, i, b, g, new16, pos16):
        old = buf[i * ROWS + b, g].reshape(8, 16, 128)
        new = jnp.broadcast_to(new16[b:b + 1, :], (16, 128)).astype(BF16)[None]
        at = jnp.broadcast_to(pos16[b:b + 1, :], (16, 128)).astype(BF16)[None]
        block = jnp.where(slot16 == at, new, old).reshape(128, 128)
        buf[i * ROWS + b, g] = block
        return block

    def score_chunk(i):
        k_in(i).wait()
        rows = chunk_ds(i)
        pos16 = t_ref[rows, :].astype(F32)
        for g in range(n_groups):
            new16 = nk_ref[g, rows, :]
            q16 = q_ref[g, rows, :]
            acc = None
            for tile in range(4):
                blk = [put_new(kbuf, i, 4 * tile + j, g, new16, pos16) for j in range(4)]
                rhs = jnp.concatenate([jnp.concatenate(blk[:2], axis=1), jnp.concatenate(blk[2:], axis=1)], axis=0)
                part = lax.dot_general(quad_lhs(q16, tile), rhs, CONTRACT_LAST, preferred_element_type=F32)
                acc = part if acc is None else acc + part
            s_ref[i % 2, g] = pick_half(acc) * scale
        k_out(i).start()

    def context_chunk(i):
        v_in(i).wait()
        rows = chunk_ds(i)
        pos16 = t_ref[rows, :]
        lane16 = lax.broadcasted_iota(jnp.int32, (ROWS, 128), 1)
        pos16f = pos16.astype(F32)
        for g in range(n_groups):
            sc = jnp.where(lane16 <= pos16, s_ref[i % 2, g], NEG_BIG)
            ex = jnp.exp(sc - jnp.max(sc, axis=-1, keepdims=True))
            prob = (ex / jnp.sum(ex, axis=-1, keepdims=True)).astype(BF16).astype(F32)
            new16 = nv_ref[g, rows, :]
            acc = None
            for tile in range(4):
                blk = [put_new(vbuf, i, 4 * tile + j, g, new16, pos16f) for j in range(4)]
                rhs = jnp.concatenate([jnp.concatenate(blk[0::2], axis=1), jnp.concatenate(blk[1::2], axis=1)], axis=0)
                part = jnp.dot(quad_lhs(prob, tile), rhs, preferred_element_type=F32)
                acc = part if acc is None else acc + part
            ctx_ref[rows, g * 128:(g + 1) * 128] = pick_half(acc).astype(BF16)
        v_out(i).start()

    score_chunk(0)

    @pl.loop(1, n_chunks)
    def _(i):
        score_chunk(i)
        context_chunk(i - 1)

    context_chunk(n_chunks - 1)

    wbig[0].wait()

    @pl.loop(0, wup_ref.shape[1] // 256)
    def _(c):
        cols = pl.ds(pl.multiple_of(c * 256, 256), 256)
        up = jnp.dot(min_ref[...], wup_ref[:, cols], preferred_element_type=F32)
        hid_ref[:, cols] = (0.5 * up * (1.0 + lax.erf(up * math.sqrt(0.5)))).astype(BF16)

    wbig[1].wait()
    wbig[2].wait()

    @pl.loop(0, d_model // 256)
    def _(c):
        cols = pl.ds(pl.multiple_of(c * 256, 256), 256)
        total = jnp.dot(hid_ref[...], wdown_ref[:, cols], preferred_element_type=F32)
        total = total + jnp.dot(ctx_ref[...], wout_ref[:, cols], preferred_element_type=F32)
        part_ref[:, cols] = total.astype(BF16)

    @pl.loop(0, n_chunks)
    def _(i):
        k_out(i).wait()
        v_out(i).wait()


N_COL = 4


def reduce_kernel(part_ref, x_hbm, out_ref, d_recv, a_send, a_recv, b_send, b_recv, keep, x_ref,
                  x_sem, d_ss, d_rs, a_ss, a_rs, b_ss, b_rs, gb_ss, gb_rs, ga_ss, ga_rs, gd_ss, gd_rs):
    me = lax.axis_index('tp')
    core = me & 1
    xpos = (me >> 1) & 1
    ypos = (me >> 2) & 1
    first_bit = jnp.where(core == 0, 2, 4)
    second_bit = 6 - first_bit
    first = me ^ first_bit
    second = me ^ second_bit
    partner = me ^ 1
    first_pos = jnp.where(core == 0, xpos, ypos)
    second_pos = jnp.where(core == 0, ypos, xpos)
    n_rows, d_model = part_ref.shape
    half, quarter, eighth = n_rows // 2, n_rows // 4, n_rows // 8
    width = d_model // N_COL

    def rows(start, size):
        return pl.ds(pl.multiple_of(start, eighth), size)

    def cols(j):
        return pl.ds(j * width, width)

    mine_half = core * half
    mine_quarter = mine_half + first_pos * quarter
    mine = mine_quarter + second_pos * eighth
    their_quarter = mine_half + (1 - first_pos) * quarter
    second_rows = mine_quarter + (1 - second_pos) * eighth

    def remote(src, dst, ss, rs, dev):
        return pltpu.make_async_remote_copy(src_ref=src, dst_ref=dst, send_sem=ss, recv_sem=rs, device_id={'tp': dev}, device_id_type=MESH)

    x_copy = pltpu.make_async_copy(x_hbm.at[rows(mine, eighth)], x_ref, x_sem)
    x_copy.start()
    barrier = pltpu.get_barrier_semaphore()
    for dev in (partner, first, second):
        pl.semaphore_signal(barrier, inc=1, device_id={'tp': dev}, device_id_type=MESH)
    pl.semaphore_wait(barrier, 3)

    d_copies, a_copies, b_copies = [], [], []
    for j in range(N_COL):
        c = remote(part_ref.at[rows((1 - core) * half, half), cols(j)], d_recv.at[:, cols(j)], d_ss.at[j], d_rs.at[j], partner)
        c.start()
        d_copies.append(c)
    for j in range(N_COL):
        d_copies[j].wait_recv()
        go = part_ref[rows(their_quarter, quarter), cols(j)].astype(F32) + d_recv[rows((1 - first_pos) * quarter, quarter), cols(j)].astype(F32)
        a_send[:, cols(j)] = go.astype(BF16)
        c = remote(a_send.at[:, cols(j)], a_recv.at[:, cols(j)], a_ss.at[j], a_rs.at[j], first)
        c.start()
        a_copies.append(c)
        keep[:, cols(j)] = part_ref[rows(mine_quarter, quarter), cols(j)].astype(F32) + d_recv[rows(first_pos * quarter, quarter), cols(j)].astype(F32)
    for j in range(N_COL):
        a_copies[j].wait_recv()
        away = rows((1 - second_pos) * eighth, eighth)
        b_send[:, cols(j)] = (keep[away, cols(j)] + a_recv[away, cols(j)].astype(F32)).astype(BF16)
        c = remote(b_send.at[:, cols(j)], b_recv.at[:, cols(j)], b_ss.at[j], b_rs.at[j], second)
        c.start()
        b_copies.append(c)
    x_copy.wait()
    gathers = []
    for j in range(N_COL):
        b_copies[j].wait_recv()
        home = rows(second_pos * eighth, eighth)
        total = keep[home, cols(j)] + a_recv[home, cols(j)].astype(F32) + b_recv[:, cols(j)].astype(F32) + x_ref[:, cols(j)].astype(F32)
        out_ref[rows(mine, eighth), cols(j)] = total.astype(BF16)
        block = out_ref.at[rows(mine, eighth), cols(j)]
        sends = [remote(block, block, gb_ss.at[j], gb_rs.at[j], second),
                 remote(block, block, ga_ss.at[j, 0], ga_rs.at[j, 0], first),
                 remote(block, block, gd_ss.at[j, 0], gd_rs.at[j, 0], partner)]
        for c in sends:
            c.start()
        gathers.append(sends)
    for j in range(N_COL):
        gathers[j][0].wait_recv()
        block = out_ref.at[rows(second_rows, eighth), cols(j)]
        sends = [remote(block, block, ga_ss.at[j, 1], ga_rs.at[j, 1], first),
                 remote(block, block, gd_ss.at[j, 1], gd_rs.at[j, 1], partner)]
        for c in sends:
            c.start()
        gathers[j] += sends
    for j in range(N_COL):
        gathers[j][1].wait_recv()
        gathers[j][3].wait_recv()
        block = out_ref.at[rows(their_quarter, quarter), cols(j)]
        c = remote(block, block, gd_ss.at[j, 2], gd_rs.at[j, 2], partner)
        c.start()
        gathers[j].append(c)
    for j in range(N_COL):
        gathers[j][2].wait_recv()
        gathers[j][4].wait_recv()
        gathers[j][5].wait_recv()
    for j in range(N_COL):
        d_copies[j].wait_send()
        a_copies[j].wait_send()
        b_copies[j].wait_send()
        for c in gathers[j]:
            c.wait_send()


def solution(mesh):
    row_spec = P('dp', None)
    vec_spec = P(None)
    cache_spec = P('dp', 'tp', None, None)
    hbm = pl.BlockSpec(memory_space=pl.ANY)
    vmem = pl.BlockSpec(memory_space=pltpu.VMEM)
    dma = pltpu.SemaphoreType.DMA

    def device_step(x, ln_attn_gamma, ln_attn_beta, ln_mlp_gamma, ln_mlp_beta, w_qkv, w_out, w_up, w_down, k_cache, v_cache, positions):
        n_rows, d_model = x.shape
        n_groups, seq, head = k_cache.shape[1:]
        ff = w_up.shape[1]
        n_chunks = n_rows // ROWS
        qkv_cols = n_groups * 3 * head
        freq = ROPE_BASE ** (-2.0 * np.arange(head // 2, dtype=np.float64) / head)
        freq = jnp.asarray(np.concatenate([freq, freq])[None, :], F32)
        w_rows = w_qkv.transpose(0, 2, 1, 3).reshape(d_model * n_groups * 3, head)
        lns = [v.reshape(1, d_model) for v in (ln_attn_gamma, ln_attn_beta, ln_mlp_gamma, ln_mlp_beta)]
        part, k_new, v_new = pl.pallas_call(
            layer_kernel,
            out_shape=(pltpu.VMEM((n_rows, d_model), BF16),
                       jax.ShapeDtypeStruct(k_cache.shape, k_cache.dtype),
                       jax.ShapeDtypeStruct(v_cache.shape, v_cache.dtype)),
            in_specs=[hbm] * 13,
            out_specs=(vmem, hbm, hbm),
            scratch_shapes=[
                pltpu.VMEM((n_rows, d_model), BF16),
                pltpu.VMEM((4, 1, d_model), F32),
                pltpu.VMEM((1, head), F32),
                pltpu.VMEM(w_rows.shape, BF16),
                pltpu.VMEM((d_model, qkv_cols), BF16),
                pltpu.VMEM((n_groups * head, d_model), BF16),
                pltpu.VMEM((d_model, ff), BF16),
                pltpu.VMEM((ff, d_model), BF16),
                pltpu.VMEM(k_cache.shape, BF16),
                pltpu.VMEM(v_cache.shape, BF16),
                pltpu.SMEM((n_rows,), jnp.int32),
                pltpu.VMEM((n_rows, d_model), BF16),
                pltpu.VMEM((n_rows, d_model), BF16),
                pltpu.VMEM((n_rows, qkv_cols), F32),
                pltpu.VMEM((n_rows, 128), jnp.int32),
                pltpu.VMEM((n_groups, n_rows, head), F32),
                pltpu.VMEM((n_groups, n_rows, head), F32),
                pltpu.VMEM((n_groups, n_rows, head), F32),
                pltpu.VMEM((2, n_groups, ROWS, seq), F32),
                pltpu.VMEM((n_rows, n_groups * head), BF16),
                pltpu.VMEM((n_rows, ff), BF16),
                pltpu.VMEM((64 * 3 * n_groups, head), F32),
                dma((8,)), dma((8,)), dma((n_chunks,)), dma((n_chunks,)), dma((n_chunks,)), dma((n_chunks,)),
            ],
            compiler_params=pltpu.CompilerParams(vmem_limit_bytes=60 * 1024 * 1024),
            cost_estimate=pl.CostEstimate(flops=4 * 10 ** 9, bytes_accessed=80 * 10 ** 6, transcendentals=0),
            name='layer',
        )(x, *lns, freq, w_rows, w_out.reshape(n_groups * head, d_model), w_up, w_down, k_cache, v_cache, positions)
        half, quarter, eighth = n_rows // 2, n_rows // 4, n_rows // 8
        out = pl.pallas_call(
            reduce_kernel,
            out_shape=jax.ShapeDtypeStruct((n_rows, d_model), BF16),
            in_specs=[vmem, hbm],
            out_specs=vmem,
            scratch_shapes=[
                pltpu.VMEM((half, d_model), BF16),
                pltpu.VMEM((quarter, d_model), BF16),
                pltpu.VMEM((quarter, d_model), BF16),
                pltpu.VMEM((eighth, d_model), BF16),
                pltpu.VMEM((eighth, d_model), BF16),
                pltpu.VMEM((quarter, d_model), F32),
                pltpu.VMEM((eighth, d_model), BF16),
                dma(()),
                dma((N_COL,)), dma((N_COL,)), dma((N_COL,)), dma((N_COL,)), dma((N_COL,)), dma((N_COL,)),
                dma((N_COL,)), dma((N_COL,)), dma((N_COL, 2)), dma((N_COL, 2)), dma((N_COL, 3)), dma((N_COL, 3)),
            ],
            compiler_params=pltpu.CompilerParams(collective_id=0, has_side_effects=True, vmem_limit_bytes=16 * 1024 * 1024),
            name='reduce',
        )(part, x)
        return out, k_new, v_new

    return jax.shard_map(device_step, mesh=mesh, in_specs=(row_spec, vec_spec, vec_spec, vec_spec, vec_spec, P(None, 'tp', None, None), P('tp', None, None, None), P(None, 'tp'), P('tp', None), cache_spec, cache_spec, P('dp')), out_specs=(row_spec, cache_spec, cache_spec), check_vma=False)
```
